128 devices in a mesh: row: 8 (over y, core), col: 16 (over z, x).
Axes of the slice: x: 4, y: 4, z: 4, core: 2. Of those that a mesh axis runs over, the one named last changes fastest.
Arguments:
- raster: float32 [256, 2048, 128], P('row', 'col'), may hold values from -6 to 6
- slot_of: int32 [256, 2048], P('row', 'col'), may hold values from 0 to 4095, as said below
- slot_target: int32 [8, 16, 4096], P('row', 'col'), may hold values from 0 to 1024, as said below
Outputs:
- parcel_means: float32 [131072, 128], P(('row', 'col'))
- anomaly: float32 [256, 2048, 128], P('row', 'col')
The draws below stay inside these ranges and needn't reach their ends.
Inputs may be any that keep to these rules, and one draw needn't show every extreme that they name: `slot_of`: A pixel's slot s is a used slot of its tile: slot_target of that tile at s is below 1024. Slot s belongs to the owner of index s // 32, numbered i * 16 + j. `slot_target`: 1024 marks an empty slot. Within one tile and one owner the used slots come first and name distinct rows; one tile may use from 1 to 32 slots of one owner; every tile fills its own block of 32 and one owner gets a full block from every tile.
All inputs are finite; a program needn't handle non-finite values.
Results may differ from the reference program's by a relative error of at most 0.00007.
Values sent between devices are 32-bit elements; how exact they have to be, the bound alone decides.
A program may use at most 64 MiB of HBM per device.

```python
import jax
import jax.numpy as jnp

BANDS = 128
TH = 32
TW = 128
PAR_DEV = 1024
CAP = 32
H = 256
W = 2048
SLOTS = 4096
PARCELS = 131072


def used_slots(key):
    devices = H // TH * (W // TW)
    counts_used = jax.random.randint(jax.random.fold_in(key, 11), (devices, devices), CAP // 4, CAP + 1)
    full_owner = jax.random.randint(jax.random.fold_in(key, 12), (), 0, devices)
    tiles = jnp.arange(devices)[:, None]
    owners = jnp.arange(devices)[None, :]
    return jnp.where((tiles == owners) | (owners == full_owner), CAP, counts_used)


def draw_slot_target(key, part):
    devices = H // TH * (W // TW)
    used = used_slots(key)
    starts = jax.random.randint(jax.random.fold_in(key, 13), (devices, devices), 0, PAR_DEV)
    offset = jnp.arange(CAP)
    target_rows = (starts[:, :, None] + offset[None, None, :]) % PAR_DEV
    target_rows = jnp.where(offset[None, None, :] < used[:, :, None], target_rows, PAR_DEV)
    return target_rows.reshape(H // TH, W // TW, devices * CAP).astype(jnp.int32)


def draw_slot_of(key, part):
    devices = H // TH * (W // TW)
    used = used_slots(key)
    tile_index = (jnp.arange(H) // TH)[:, None] * (W // TW) + (jnp.arange(W) // TW)[None, :]
    owners = jax.random.randint(jax.random.fold_in(key, 14), (H, W), 0, devices)
    limit = used[tile_index, owners]
    within = jax.random.randint(jax.random.fold_in(key, 15), (H, W), 0, 1 << 20) % limit
    return (owners * CAP + within).astype(jnp.int32)


def shard_levels(rng, dims, pieces, low, largest):
    loudness = 1.0
    for position, shards_of in pieces:
        steps = jax.random.uniform(jax.random.fold_in(jax.random.fold_in(rng, 6), position), (shards_of,), jnp.float32, low / len(pieces), largest / len(pieces))
        loudness = loudness * jnp.repeat(jnp.exp(steps), dims[position] // shards_of).reshape((-1,) + (1,) * (len(dims) - 1 - position))
    return loudness


def gaussian(own_key, dims, deviation, most, pieces=(), kind=jnp.bfloat16):
    loudness = shard_levels(own_key, dims, pieces, -0.22, 0.18) if pieces else 1.0
    drawn = jax.random.normal(own_key, dims, jnp.float32) * deviation * loudness
    return jnp.minimum(jnp.maximum(drawn, -most), most).astype(kind)


def setup_inputs(seed: int = 0) -> dict:
    key_of = jax.random.split(jax.random.key(seed), 4)
    raster = gaussian(key_of[0], (H, W, BANDS), 1.0, 6.0, ((0, 8), (1, 16)), jnp.float32)
    slot_of = draw_slot_of(jax.random.fold_in(key_of[3], 71), 0)
    slot_target = draw_slot_target(jax.random.fold_in(key_of[3], 71), 0)
    return {"raster": raster, "slot_of": slot_of, "slot_target": slot_target}


def reference(raster, slot_of, slot_target):
    tile_index = (jnp.arange(H, dtype=jnp.int32) // TH)[:, None] * (W // TW) + (jnp.arange(W, dtype=jnp.int32) // TW)[None, :]
    targets_all = slot_target.reshape(-1, SLOTS)
    row_at = targets_all[tile_index, slot_of]
    owner_index = slot_of // CAP
    parcel_index = jnp.where(row_at < PAR_DEV, owner_index * PAR_DEV + row_at, PARCELS).astype(jnp.int32)
    flat_index = parcel_index.reshape(-1)
    flat_pixels = raster.reshape(H * W, BANDS)
    parcel_sums = jax.ops.segment_sum(flat_pixels, flat_index, PARCELS + 1)
    parcel_counts = jax.ops.segment_sum(jnp.ones((H * W,), jnp.float32), flat_index, PARCELS + 1)
    parcel_means = parcel_sums[:PARCELS] / jnp.maximum(parcel_counts[:PARCELS], 1.0)[:, None]
    padded = jnp.concatenate([parcel_means, jnp.zeros((1, BANDS), jnp.float32)], axis=0)
    anomaly = raster - padded[flat_index].reshape(H, W, BANDS)
    return parcel_means, anomaly
```

```python
import itertools

import jax
import jax.numpy as jnp
from jax import lax
from jax.experimental import pallas as pl
from jax.experimental.pallas import tpu as pltpu
from jax.sharding import PartitionSpec as P

MESH = pl.DeviceIdType.MESH
PIX = 4096
BANDS = 128
PAR_DEV = 1024
CAP = 32
DEVS = 128
BLK = 8
ROWS = BLK * CAP
BATCHES = DEVS // BLK
EARLY = 2
BF = jnp.bfloat16
F32 = jnp.float32
I16 = jnp.int16


def _hops(d):
    return sum(min(v, 4 - v) for v in d)


ORDER = sorted(itertools.product(range(4), repeat=3), key=lambda d: (-_hops(d),) + d)
CODES = [d[0] + 4 * d[1] + 16 * d[2] for d in ORDER]


def pick(values, index):
    got = jnp.int32(values[0])
    for n, v in enumerate(values[1:], 1):
        got = jnp.where(index == n, jnp.int32(v), got)
    return got


def split(v):
    hi = v.astype(BF)
    lo = (v - hi.astype(F32)).astype(BF)
    return hi, lo


def onehot(mask):
    return jnp.where(mask, jnp.ones((), BF), jnp.zeros((), BF))


def kernel(
    raster, slots, targets, tot, acc,
    x2, oh, b1, rowb, colb, tcol, inv, m2,
    send, got, rep, ret, small_out, small_in, slot_v, targ_v,
    s_in, s_send, s_got, s_small, s_ret,
):
    row, col = lax.axis_index("row"), lax.axis_index("col")
    x, y, z, core = col % 4, row // 2, col // 4, row % 2
    me = row * 16 + col

    def place(code, sign):
        dx, dy, dz = code % 4, (code // 4) % 4, code // 16
        return (x + sign * dx + 4) % 4, (y + sign * dy + 4) % 4, (z + sign * dz + 4) % 4

    def lin(tx, ty, tz, tc):
        return (ty * 2 + tc) * 16 + tz * 4 + tx

    def remote(src, dst, send_sem, recv_sem, t):
        tx, ty, tz, tc = t
        pltpu.make_async_remote_copy(
            src_ref=src, dst_ref=dst, send_sem=send_sem, recv_sem=recv_sem,
            device_id=(ty * 2 + tc, tz * 4 + tx), device_id_type=MESH,
        ).start()

    def send_or_keep(src, dst, send_sem, recv_sem, t, may_be_self):
        if not may_be_self:
            remote(src, dst, send_sem, recv_sem, t)
            return
        mine = lin(*t) == me

        @pl.when(jnp.logical_not(mine))
        def _():
            remote(src, dst, send_sem, recv_sem, t)

        @pl.when(mine)
        def _():
            pltpu.make_async_copy(src, dst, recv_sem).start()

    def wait_bytes(ref, sem):
        pltpu.make_async_copy(ref, ref, sem).wait()

    in_slots = pltpu.make_async_copy(slots, slot_v, s_in.at[0])
    in_targets = pltpu.make_async_copy(targets, targ_v, s_in.at[1])
    in_slots.start()
    in_targets.start()
    quarter = PIX // 4
    in_raster = []
    for n in range(4):
        part = pl.ds(n * quarter, quarter)
        in_raster.append(pltpu.make_async_copy(raster.at[part], acc.at[part], s_in.at[2 + n]))
        in_raster[-1].start()
    barrier = pltpu.get_barrier_semaphore()

    def greet(n, carry):
        t = (me + n) % DEVS
        pl.semaphore_signal(barrier, inc=1, device_id=(t // 16, t % 16), device_id_type=MESH)
        return carry

    lax.fori_loop(1, DEVS, greet, 0)

    in_slots.wait()
    for r in range(32):
        rowb[16 * r : 16 * r + 16, :] = jnp.broadcast_to(slot_v[r : r + 1, :], (16, 128)).astype(I16)
    for n in range(4):
        in_raster[n].wait()
        for h in range(4):
            a = n * quarter + h * 256
            hi, lo = split(acc[a : a + 256, :])
            x2[a : a + 256, 0:128] = hi
            x2[a : a + 256, 128:256] = lo

    iota32 = lax.broadcasted_iota(jnp.int32, (32, 128), 0)

    def sum_batch(b):
        g, bb = b // 8, b % 8
        places = [place(pick(CODES[k::8], bb), 1) + (g,) for k in range(BLK)]
        ids = jnp.concatenate([(iota32 + lin(*t) * CAP).astype(I16) for t in places], axis=0)
        ids = ids.reshape(16, 16, 128)
        for r in range(32):
            m = rowb[16 * r : 16 * r + 16, :][None] == ids
            oh[:, 128 * r : 128 * r + 128] = onehot(m).reshape(ROWS, 128)
        s = jnp.dot(oh[...], x2[...], preferred_element_type=F32)
        send[pl.ds(pl.multiple_of(b * ROWS, ROWS), ROWS), :] = s[:, :128] + s[:, 128:]

    def send_batch(b):
        g, bb = b // 8, b % 8
        for k in range(BLK):
            i = bb * 8 + k
            t = place(pick(CODES[k::8], bb), 1) + (g,)
            src = send.at[pl.ds(pl.multiple_of((b * 8 + k) * CAP, CAP), CAP)]
            dst = got.at[pl.ds(pl.multiple_of((i * 2 + core) * CAP, CAP), CAP)]
            send_or_keep(src, dst, s_send.at[0], s_got.at[bb * 2 + k // 4], t, k == 7)

    for b in range(EARLY):
        sum_batch(b)
    pl.semaphore_wait(barrier, DEVS - 1)
    for b in range(EARLY):
        send_batch(b)

    pad = jnp.zeros((96, 128), jnp.int32)
    turned = jnp.concatenate([slot_v[...], pad], axis=0).T
    lane16 = lax.broadcasted_iota(jnp.int32, (128, 128), 1).astype(I16)
    for r in range(32):
        c = jnp.broadcast_to(turned[:, r : r + 1], (128, 128))
        colb[128 * r : 128 * r + 128, :] = c.astype(I16)
        b1[128 * r : 128 * r + 128, :] = onehot((c % 128).astype(I16) == lane16)
        hi_row = jnp.broadcast_to(slot_v[r : r + 1, :] // 128, (32, 128)).astype(I16)
        oh[0:32, 128 * r : 128 * r + 128] = onehot(hi_row == iota32.astype(I16))
    counts = jnp.dot(oh[0:32, :], b1[...], preferred_element_type=F32)
    in_targets.wait()
    targ = targ_v[...].astype(F32)
    lane = lax.broadcasted_iota(jnp.int32, (32, 128), 1)
    for m in range(4):
        t = pltpu.roll(targ, (128 - 32 * m) % 128, 1)
        c = pltpu.roll(counts, (128 + 32 - 32 * m) % 128, 1)
        v = jnp.where(lane < 32, t, jnp.where(lane < 64, c, 0.0))
        small_out[pl.ds(m, 32, stride=4), :] = v

    def send_small(i, carry):
        code = pick(CODES, i)
        for g in range(2):
            t = place(code, 1) + (g,)
            src = small_out.at[pl.ds(lin(*t), 1)]
            dst = small_in.at[pl.ds(i * 2 + core, 1)]
            send_or_keep(src, dst, s_send.at[1], s_small.at[0], t, True)
        return carry

    lax.fori_loop(0, 64, send_small, 0)

    def batch(b, carry):
        sum_batch(b)
        send_batch(b)
        return carry

    lax.fori_loop(EARLY, BATCHES, batch, 0)

    wait_bytes(small_in, s_small.at[0])
    t_all = jnp.zeros((32, 128), F32)
    c_all = jnp.zeros((32, 128), F32)
    for m in range(4):
        v = small_in[pl.ds(m, 32, stride=4), :]
        group = lane // 32 == m
        t_all = jnp.where(group, pltpu.roll(v, (32 * m) % 128, 1), t_all)
        c_all = jnp.where(group, pltpu.roll(v, (128 + 32 * m - 32) % 128, 1), c_all)
    targ_v[...] = t_all.astype(jnp.int32)
    slot_v[...] = c_all.astype(jnp.int32)
    turned = jnp.concatenate([targ_v[...], pad], axis=0).T
    for r in range(32):
        rowb[16 * r : 16 * r + 16, :] = jnp.broadcast_to(targ_v[r : r + 1, :], (16, 128)).astype(I16)
        tcol[128 * r : 128 * r + 128, :] = jnp.broadcast_to(turned[:, r : r + 1], (128, 128)).astype(I16)

    iota64 = lax.broadcasted_iota(jnp.int32, (64, 128), 0)

    def number(n, carry):
        ids = iota64 + n * 64
        s = jnp.zeros((64, 128), F32)
        for r in range(32):
            m = jnp.broadcast_to(targ_v[r : r + 1, :], (64, 128)) == ids
            c = jnp.broadcast_to(slot_v[r : r + 1, :], (64, 128)).astype(F32)
            s = s + jnp.where(m, c, 0.0)
        s = jnp.sum(s, axis=1, keepdims=True)
        here = pl.ds(pl.multiple_of(n * 64, 64), 64)
        inv[here, :] = jnp.broadcast_to(1.0 / jnp.maximum(s, 1.0), (64, 128))
        tot[here, :] = jnp.zeros((64, 128), F32)
        return carry

    lax.fori_loop(0, PAR_DEV // 64, number, 0)

    iota256 = lax.broadcasted_iota(jnp.int32, (256, 128), 0)

    def gather_sums(b, carry):
        here = pl.ds(pl.multiple_of(b * ROWS, ROWS), ROWS)
        wait_bytes(got.at[here], s_got.at[b])
        r2 = jnp.concatenate(split(got[here, :]), axis=1)
        rows = [rowb[pl.ds(pl.multiple_of((2 * b + h) * 16, 16), 16), :][None] for h in range(2)]
        for n in range(4):
            ids = (iota256 + n * 256).astype(I16).reshape(16, 16, 128)
            table = jnp.concatenate([onehot(v == ids).reshape(256, 128) for v in rows], axis=1)
            s = jnp.dot(table, r2, preferred_element_type=F32)
            tot[n * 256 : n * 256 + 256, :] += s[:, :128] + s[:, 128:]
        return carry

    lax.fori_loop(0, BATCHES, gather_sums, 0)

    for n in range(4):
        part = slice(n * 256, n * 256 + 256)
        mean = tot[part, :] * inv[part, :]
        tot[part, :] = mean
        hi, lo = split(mean)
        m2[part, 0:128] = hi
        m2[part, 128:256] = lo

    lane256 = lax.broadcasted_iota(jnp.int32, (256, 128), 1)

    def reply(b, carry):
        here = pl.ds(pl.multiple_of(b * ROWS, ROWS), ROWS)
        wanted = tcol[here, :]
        table = jnp.concatenate(
            [onehot(wanted == (lane256 + 128 * n).astype(I16)) for n in range(8)], axis=1
        )
        s = jnp.dot(table, m2[...], preferred_element_type=F32)
        rep[here, :] = s[:, :128] + s[:, 128:]
        for k in range(4):
            i = b * 4 + k
            chip = place(pick(CODES[k::4], b), -1)
            for g in range(2):
                src = rep.at[pl.ds(pl.multiple_of((i * 2 + g) * CAP, CAP), CAP)]
                dst = ret.at[pl.ds(pl.multiple_of((core * 64 + i) * CAP, CAP), CAP)]
                send_or_keep(src, dst, s_send.at[2], s_ret.at[core * 8 + b // 2], chip + (g,), k == 3)
        return carry

    lax.fori_loop(0, BATCHES, reply, 0)

    lane16r = lax.broadcasted_iota(jnp.int32, (16, 128), 1)

    def subtract(n, r2, ids):
        part = pl.ds(pl.multiple_of(n * 256, 256), 256)
        px = colb[part, :].reshape(16, 16, 128)
        table = jnp.concatenate([onehot(px == v).reshape(256, 128) for v in ids], axis=1)
        s = jnp.dot(table, r2, preferred_element_type=F32)
        acc[part, :] = acc[part, :] - s[:, :128] - s[:, 128:]

    def read_batch(b, carry):
        here = pl.ds(pl.multiple_of(b * ROWS, ROWS), ROWS)
        g, bb = b // 8, b % 8
        ids = []
        for h in range(2):
            v = lane16r % 32
            for m in range(4):
                base = lin(*place(pick(CODES[4 * h + m :: 8], bb), 1), g) * CAP
                v = v + jnp.where(lane16r // 32 == m, base, 0)
            ids.append(v.astype(I16)[None])
        wait_bytes(ret.at[here], s_ret.at[b])
        r2 = jnp.concatenate(split(ret[here, :]), axis=1)
        for n in range(16):
            subtract(n, r2, ids)
        return carry

    lax.fori_loop(0, BATCHES, read_batch, 0)

    most = pl.ds(0, (DEVS - 1) * CAP)
    wait_bytes(send.at[most], s_send.at[0])
    wait_bytes(small_out.at[pl.ds(0, DEVS - 1)], s_send.at[1])
    wait_bytes(rep.at[most], s_send.at[2])


def per_device(raster, slot_of, slot_target):
    operands = (raster.reshape(PIX, BANDS), slot_of, slot_target.reshape(32, 128))
    here = pl.BlockSpec(memory_space=pltpu.VMEM)
    outside = pl.BlockSpec(memory_space=pltpu.HBM)
    table = pltpu.VMEM((PIX, BANDS), F32)
    means, anomaly = pl.pallas_call(
        kernel,
        out_shape=(
            jax.ShapeDtypeStruct((PAR_DEV, BANDS), F32),
            jax.ShapeDtypeStruct((PIX, BANDS), F32),
        ),
        in_specs=[outside] * 3,
        out_specs=(here, here),
        scratch_shapes=[
            pltpu.VMEM((PIX, 2 * BANDS), BF),
            pltpu.VMEM((ROWS, PIX), BF),
            pltpu.VMEM((PIX, 128), BF),
            pltpu.VMEM((512, 128), I16),
            pltpu.VMEM((PIX, 128), I16),
            pltpu.VMEM((PIX, 128), I16),
            pltpu.VMEM((PAR_DEV, BANDS), F32),
            pltpu.VMEM((PAR_DEV, 2 * BANDS), BF),
            table,
            table,
            table,
            table,
            pltpu.VMEM((DEVS, 128), F32),
            pltpu.VMEM((DEVS, 128), F32),
            pltpu.VMEM((32, 128), jnp.int32),
            pltpu.VMEM((32, 128), jnp.int32),
            pltpu.SemaphoreType.DMA((6,)),
            pltpu.SemaphoreType.DMA((3,)),
            pltpu.SemaphoreType.DMA((BATCHES,)),
            pltpu.SemaphoreType.DMA((1,)),
            pltpu.SemaphoreType.DMA((BATCHES,)),
        ],
        compiler_params=pltpu.CompilerParams(
            collective_id=0, has_side_effects=True, vmem_limit_bytes=48 * 2**20
        ),
    )(*(pltpu.with_memory_space_constraint(v, pltpu.HBM) for v in operands))
    return means, anomaly.reshape(raster.shape)


def solution(mesh):
    placed = (P("row", "col", None), P("row", "col"), P("row", "col", None))
    return jax.shard_map(
        per_device,
        mesh=mesh,
        in_specs=placed,
        out_specs=(P(("row", "col"), None), P("row", "col", None)),
        check_vma=False,
    )
```

```python
import itertools
import random

import jax
import jax.numpy as jnp
from jax import lax
from jax.experimental import pallas as pl
from jax.experimental.pallas import tpu as pltpu
from jax.sharding import PartitionSpec as P

MESH = pl.DeviceIdType.MESH
PIX = 4096
BANDS = 128
PAR_DEV = 1024
CAP = 32
MSG = CAP + 1
STEP = 40
DEVS = 128
BLK = 8
ROWS = BLK * CAP
BATCHES = DEVS // BLK
EARLY = 2
BF = jnp.bfloat16
F32 = jnp.float32
I16 = jnp.int16


ORDER = [d for d in itertools.product(range(4), repeat=3) if any(d)]
random.Random(0).shuffle(ORDER)
ORDER.append((0, 0, 0))
CODES = [d[0] + 4 * d[1] + 16 * d[2] for d in ORDER]


def pick(values, index):
    got = jnp.int32(values[0])
    for n, v in enumerate(values[1:], 1):
        got = jnp.where(index == n, jnp.int32(v), got)
    return got


def split(v):
    hi = v.astype(BF)
    lo = (v - hi.astype(F32)).astype(BF)
    return hi, lo


def onehot(mask):
    return jnp.where(mask, jnp.ones((), BF), jnp.zeros((), BF))


def over_rows(v):
    v = jnp.broadcast_to(v, (16, 128)).astype(I16)
    return jnp.concatenate([v] * 16, axis=0)


def kernel(
    raster, slots, targets, tot, acc,
    x2, b1, colb, tcol, num, m2,
    send, got, rep, ret, small, slot_v, targ_v,
    s_in, s_send, s_got, s_ret,
):
    row, col = lax.axis_index("row"), lax.axis_index("col")
    x, y, z, core = col % 4, row // 2, col // 4, row % 2
    me = row * 16 + col

    def place(code, sign):
        dx, dy, dz = lax.rem(code, 4), lax.rem(lax.div(code, 4), 4), lax.div(code, 16)
        return tuple(lax.rem(v + sign * d + 4, 4) for v, d in ((x, dx), (y, dy), (z, dz)))

    def lin(tx, ty, tz, tc):
        return (ty * 2 + tc) * 16 + tz * 4 + tx

    def remote(src, dst, send_sem, recv_sem, t):
        tx, ty, tz, tc = t
        pltpu.make_async_remote_copy(
            src_ref=src, dst_ref=dst, send_sem=send_sem, recv_sem=recv_sem,
            device_id=(ty * 2 + tc, tz * 4 + tx), device_id_type=MESH,
        ).start()

    def send_or_keep(src, dst, send_sem, recv_sem, t, may_be_self):
        if not may_be_self:
            remote(src, dst, send_sem, recv_sem, t)
            return
        mine = lin(*t) == me

        @pl.when(jnp.logical_not(mine))
        def _():
            remote(src, dst, send_sem, recv_sem, t)

        @pl.when(mine)
        def _():
            pltpu.make_async_copy(src, dst, recv_sem).start()

    def wait_bytes(ref, sem):
        pltpu.make_async_copy(ref, ref, sem).wait()

    in_slots = pltpu.make_async_copy(slots, slot_v, s_in.at[0])
    in_targets = pltpu.make_async_copy(targets, targ_v, s_in.at[1])
    in_slots.start()
    in_targets.start()
    quarter = PIX // 4
    in_raster = []
    for n in range(4):
        part = pl.ds(n * quarter, quarter)
        in_raster.append(pltpu.make_async_copy(raster.at[part], acc.at[part], s_in.at[2 + n]))
        in_raster[-1].start()
    barrier = pltpu.get_barrier_semaphore()

    def greet(n, carry):
        far = (row + n) % 8
        for k in range(16):
            there = (far, (col + k) % 16)
            pl.semaphore_signal(barrier, inc=1, device_id=there, device_id_type=MESH)
        return carry

    for k in range(1, 16):
        there = (row, (col + k) % 16)
        pl.semaphore_signal(barrier, inc=1, device_id=there, device_id_type=MESH)
    lax.fori_loop(1, 8, greet, 0)

    in_slots.wait()
    iota32 = lax.broadcasted_iota(jnp.int32, (32, 128), 0)

    pad = jnp.zeros((96, 128), jnp.int32)
    turned = jnp.concatenate([slot_v[...], pad], axis=0).T
    lane16 = lax.broadcasted_iota(jnp.int32, (128, 128), 1).astype(I16)
    table = []
    for r in range(32):
        c = jnp.broadcast_to(turned[:, r : r + 1], (128, 128))
        colb[128 * r : 128 * r + 128, :] = c
        b1[128 * r : 128 * r + 128, :] = onehot((c % 128).astype(I16) == lane16)
        high = jnp.broadcast_to(slot_v[r : r + 1, :] // 128, (32, 128)).astype(I16)
        table.append(onehot(high == iota32.astype(I16)))
    counts = jnp.dot(jnp.concatenate(table, axis=1), b1[...], preferred_element_type=F32)
    in_targets.wait()
    targ = targ_v[...].astype(F32)
    lane = lax.broadcasted_iota(jnp.int32, (32, 128), 1)
    for m in range(4):
        t = pltpu.roll(targ, (128 - 32 * m) % 128, 1)
        c = pltpu.roll(counts, (128 + 32 - 32 * m) % 128, 1)
        v = jnp.where(lane < 32, t, jnp.where(lane < 64, c, 0.0))
        small[pl.ds(m, 32, stride=4), :] = v

    for n in range(4):
        in_raster[n].wait()
        for h in range(4):
            a = n * quarter + h * 256
            hi, lo = split(acc[a : a + 256, :])
            x2[a : a + 256, 0:128] = hi
            x2[a : a + 256, 128:256] = lo

    def sum_batch(b):
        g, bb = lax.div(b, 8), lax.rem(b, 8)
        places = [place(pick(CODES[k::8], bb), 1) + (g,) for k in range(BLK)]
        ids = jnp.concatenate([(iota32 + lin(*t) * CAP).astype(I16) for t in places], axis=0)
        table = [onehot(over_rows(slot_v[r : r + 1, :]) == ids) for r in range(32)]
        s = jnp.dot(jnp.concatenate(table, axis=1), x2[...], preferred_element_type=F32)
        s = s[:, :128] + s[:, 128:]
        for k in range(BLK):
            at = (b * 8 + k) * STEP
            send[pl.ds(pl.multiple_of(at, 8), CAP), :] = s[k * CAP : k * CAP + CAP, :]
            send[pl.ds(at + CAP, 1), :] = small[pl.ds(lin(*places[k]), 1), :]

    def send_batch(b):
        g, bb = lax.div(b, 8), lax.rem(b, 8)
        for k in range(BLK):
            i = bb * 8 + k
            t = place(pick(CODES[k::8], bb), 1) + (g,)
            src = send.at[pl.ds(pl.multiple_of((b * 8 + k) * STEP, 8), MSG)]
            dst = got.at[pl.ds(pl.multiple_of((core * 64 + i) * STEP, 8), MSG)]
            send_or_keep(src, dst, s_send.at[0], s_got.at[core * 8 + bb], t, k == 7)

    def first(b, carry):
        sum_batch(b)
        return carry

    def then_send(b, carry):
        send_batch(b)
        return carry

    lax.fori_loop(0, EARLY, first, 0)
    pl.semaphore_wait(barrier, DEVS - 1)
    lax.fori_loop(0, EARLY, then_send, 0)

    def batch(b, carry):
        sum_batch(b)
        send_batch(b)
        return carry

    lax.fori_loop(EARLY, BATCHES, batch, 0)

    for n in range(4):
        part = slice(n * 256, n * 256 + 256)
        tot[part, :] = jnp.zeros((256, 128), F32)
        num[part, :] = jnp.zeros((256, 128), F32)
    iota256 = lax.broadcasted_iota(jnp.int32, (256, 128), 0)
    sub8 = lax.broadcasted_iota(jnp.int32, (8, 128), 0)
    lane8 = lax.broadcasted_iota(jnp.int32, (8, 128), 1)

    def in_lanes(v, first):
        w = jnp.zeros((8, 128), F32)
        for m in range(4):
            here = (lane8 // 32 == m) & (sub8 % 4 == m)
            w = jnp.where(here, pltpu.roll(v, (128 + 32 * m - first) % 128, 1), w)
        return [jnp.sum(w[4 * h : 4 * h + 4, :], axis=0, keepdims=True) for h in range(2)]

    def gather_sums(n, carry):
        b = (n % 2) * 8 + n // 2
        at = b * BLK * STEP
        wait_bytes(got.at[pl.ds(pl.multiple_of(at, 8), BLK * MSG)], s_got.at[b])
        block = [got[pl.ds(pl.multiple_of(at + k * STEP, 8), CAP), :] for k in range(BLK)]
        r2 = jnp.concatenate(split(jnp.concatenate(block, axis=0)), axis=1)
        extra = [got[pl.ds(at + k * STEP + CAP, 1), :] for k in range(BLK)]
        extra = jnp.concatenate(extra, axis=0)
        wanted = [v.astype(jnp.int32) for v in in_lanes(extra, 0)]
        counts = in_lanes(extra, CAP)
        turned = jnp.concatenate(wanted + [jnp.zeros((6, 128), jnp.int32)], axis=0).T
        for h in range(2):
            column = jnp.broadcast_to(turned[:, h : h + 1], (128, 128))
            tcol[pl.ds(pl.multiple_of(b * ROWS + h * 128, 128), 128), :] = column
        rows = [over_rows(v) for v in wanted]
        for n in range(4):
            part = slice(n * 256, n * 256 + 256)
            ids = iota256 + n * 256
            c = num[part, :]
            for h in range(2):
                c = c + jnp.where(wanted[h] == ids, counts[h], 0.0)
            num[part, :] = c
            table = jnp.concatenate([onehot(v == ids.astype(I16)) for v in rows], axis=1)
            s = jnp.dot(table, r2, preferred_element_type=F32)
            tot[part, :] += s[:, :128] + s[:, 128:]
        return carry

    lax.fori_loop(0, BATCHES, gather_sums, 0)

    for n in range(4):
        part = slice(n * 256, n * 256 + 256)
        number = jnp.sum(num[part, :], axis=1, keepdims=True)
        mean = tot[part, :] * (1.0 / jnp.maximum(number, 1.0))
        tot[part, :] = mean
        hi, lo = split(mean)
        m2[part, 0:128] = hi
        m2[part, 128:256] = lo

    lane256 = lax.broadcasted_iota(jnp.int32, (256, 128), 1)

    def reply(n, carry):
        g, bb = (core + n // 8) % 2, n % 8
        b = g * 8 + bb
        here = pl.ds(pl.multiple_of(b * ROWS, ROWS), ROWS)
        wanted = tcol[here, :].astype(I16)
        table = jnp.concatenate(
            [onehot(wanted == (lane256 + 128 * n).astype(I16)) for n in range(8)], axis=1
        )
        s = jnp.dot(table, m2[...], preferred_element_type=F32)
        rep[here, :] = s[:, :128] + s[:, 128:]
        for k in range(BLK):
            i = bb * 8 + k
            t = place(pick(CODES[k::8], bb), -1) + (g,)
            src = rep.at[pl.ds(pl.multiple_of((b * 8 + k) * CAP, CAP), CAP)]
            dst = ret.at[pl.ds(pl.multiple_of((core * 64 + i) * CAP, CAP), CAP)]
            send_or_keep(src, dst, s_send.at[1], s_ret.at[core * 8 + bb], t, k == 7)
        return carry

    lax.fori_loop(0, BATCHES, reply, 0)

    lane1 = lax.broadcasted_iota(jnp.int32, (1, 128), 1)

    def subtract(n, r2, ids):
        part = pl.ds(pl.multiple_of(n * 256, 256), 256)
        px = colb[part, :].astype(I16)
        table = jnp.concatenate([onehot(px == v) for v in ids], axis=1)
        s = jnp.dot(table, r2, preferred_element_type=F32)
        acc[part, :] = acc[part, :] - s[:, :128] - s[:, 128:]

    def read_batch(b, carry):
        here = pl.ds(pl.multiple_of(b * ROWS, ROWS), ROWS)
        g, bb = lax.div(b, 8), lax.rem(b, 8)
        ids = []
        for h in range(2):
            v = lane1 % 32
            for m in range(4):
                base = lin(*place(pick(CODES[4 * h + m :: 8], bb), 1), g) * CAP
                v = v + jnp.where(lane1 // 32 == m, base, 0)
            ids.append(over_rows(v))
        wait_bytes(ret.at[here], s_ret.at[b])
        r2 = jnp.concatenate(split(ret[here, :]), axis=1)
        for n in range(16):
            subtract(n, r2, ids)
        return carry

    lax.fori_loop(0, BATCHES, read_batch, 0)

    wait_bytes(send.at[pl.ds(0, (DEVS - 1) * MSG)], s_send.at[0])
    wait_bytes(rep.at[pl.ds(0, (DEVS - 1) * CAP)], s_send.at[1])


def per_device(raster, slot_of, slot_target):
    operands = (raster.reshape(PIX, BANDS), slot_of, slot_target.reshape(32, 128))
    here = pl.BlockSpec(memory_space=pltpu.VMEM)
    outside = pl.BlockSpec(memory_space=pltpu.HBM)
    table = pltpu.VMEM((PIX, BANDS), F32)
    means, anomaly = pl.pallas_call(
        kernel,
        out_shape=(
            jax.ShapeDtypeStruct((PAR_DEV, BANDS), F32),
            jax.ShapeDtypeStruct((PIX, BANDS), F32),
        ),
        in_specs=[outside] * 3,
        out_specs=(here, here),
        scratch_shapes=[
            pltpu.VMEM((PIX, 2 * BANDS), BF),
            pltpu.VMEM((PIX, 128), BF),
            pltpu.VMEM((PIX, 128), jnp.int32),
            pltpu.VMEM((PIX, 128), jnp.int32),
            pltpu.VMEM((PAR_DEV, BANDS), F32),
            pltpu.VMEM((PAR_DEV, 2 * BANDS), BF),
            pltpu.VMEM((DEVS * STEP, BANDS), F32),
            pltpu.VMEM((DEVS * STEP, BANDS), F32),
            table,
            table,
            pltpu.VMEM((DEVS, 128), F32),
            pltpu.VMEM((32, 128), jnp.int32),
            pltpu.VMEM((32, 128), jnp.int32),
            pltpu.SemaphoreType.DMA((6,)),
            pltpu.SemaphoreType.DMA((2,)),
            pltpu.SemaphoreType.DMA((BATCHES,)),
            pltpu.SemaphoreType.DMA((BATCHES,)),
        ],
        compiler_params=pltpu.CompilerParams(
            collective_id=0, has_side_effects=True, vmem_limit_bytes=48 * 2**20
        ),
    )(*(pltpu.with_memory_space_constraint(v, pltpu.HBM) for v in operands))
    return means, anomaly.reshape(raster.shape)


def solution(mesh):
    placed = (P("row", "col", None), P("row", "col"), P("row", "col", None))
    return jax.shard_map(
        per_device,
        mesh=mesh,
        in_specs=placed,
        out_specs=(P(("row", "col"), None), P("row", "col", None)),
        check_vma=False,
    )
```

```python
import itertools

import jax
import jax.numpy as jnp
from jax import lax
from jax.experimental import pallas as pl
from jax.experimental.pallas import tpu as pltpu
from jax.sharding import PartitionSpec as P

MESH = pl.DeviceIdType.MESH
PIX = 4096
BANDS = 128
PAR_DEV = 1024
CAP = 32
MSG = CAP + 1
STEP = 40
DEVS = 128
BLK = 8
ROWS = BLK * CAP
BATCHES = DEVS // BLK
EARLY = 2
BF = jnp.bfloat16
F32 = jnp.float32
I16 = jnp.int16


SHIFTS = list(itertools.product(range(4), repeat=2))
ORDER = [(t, (t + u) % 4, (t + v) % 4) for u, v in SHIFTS[1:] + SHIFTS[:1] for t in (2, 1, 3, 0)]
CODES = [d[0] + 4 * d[1] + 16 * d[2] for d in ORDER]


def pick(values, index):
    got = jnp.int32(values[0])
    for n, v in enumerate(values[1:], 1):
        got = jnp.where(index == n, jnp.int32(v), got)
    return got


def split(v):
    hi = v.astype(BF)
    lo = (v - hi.astype(F32)).astype(BF)
    return hi, lo


def onehot(mask):
    return jnp.where(mask, jnp.ones((), BF), jnp.zeros((), BF))


def over_rows(v):
    v = jnp.broadcast_to(v, (16, 128)).astype(I16)
    return jnp.concatenate([v] * 16, axis=0)


def kernel(
    raster, slots, targets, tot, acc,
    x2, b1, colb, tcol, num, m2,
    send, got, rep, ret, small, slot_v, targ_v,
    s_in, s_send, s_got, s_ret,
):
    row, col = lax.axis_index("row"), lax.axis_index("col")
    x, y, z, core = col % 4, row // 2, col // 4, row % 2
    me = row * 16 + col

    def place(code, sign):
        dx, dy, dz = lax.rem(code, 4), lax.rem(lax.div(code, 4), 4), lax.div(code, 16)
        return tuple(lax.rem(v + sign * d + 4, 4) for v, d in ((x, dx), (y, dy), (z, dz)))

    def lin(tx, ty, tz, tc):
        return (ty * 2 + tc) * 16 + tz * 4 + tx

    def remote(src, dst, send_sem, recv_sem, t):
        tx, ty, tz, tc = t
        pltpu.make_async_remote_copy(
            src_ref=src, dst_ref=dst, send_sem=send_sem, recv_sem=recv_sem,
            device_id=(ty * 2 + tc, tz * 4 + tx), device_id_type=MESH,
        ).start()

    def send_or_keep(src, dst, send_sem, recv_sem, t, may_be_self):
        if not may_be_self:
            remote(src, dst, send_sem, recv_sem, t)
            return
        mine = lin(*t) == me

        @pl.when(jnp.logical_not(mine))
        def _():
            remote(src, dst, send_sem, recv_sem, t)

        @pl.when(mine)
        def _():
            pltpu.make_async_copy(src, dst, recv_sem).start()

    def wait_bytes(ref, sem):
        pltpu.make_async_copy(ref, ref, sem).wait()

    in_slots = pltpu.make_async_copy(slots, slot_v, s_in.at[0])
    in_targets = pltpu.make_async_copy(targets, targ_v, s_in.at[1])
    in_slots.start()
    in_targets.start()
    quarter = PIX // 4
    in_raster = []
    for n in range(4):
        part = pl.ds(n * quarter, quarter)
        in_raster.append(pltpu.make_async_copy(raster.at[part], acc.at[part], s_in.at[2 + n]))
        in_raster[-1].start()
    barrier = pltpu.get_barrier_semaphore()

    around = [(k + 10) % 16 for k in range(16)]

    def greet(n, carry):
        far = lax.rem(row + n, 8)
        for k in around:
            there = (far, lax.rem(col + k, 16))
            pl.semaphore_signal(barrier, inc=1, device_id=there, device_id_type=MESH)
        return carry

    lax.fori_loop(4, 8, greet, 0)
    lax.fori_loop(1, 4, greet, 0)
    for k in around:
        if k:
            there = (row, lax.rem(col + k, 16))
            pl.semaphore_signal(barrier, inc=1, device_id=there, device_id_type=MESH)

    in_slots.wait()
    iota32 = lax.broadcasted_iota(jnp.int32, (32, 128), 0)

    pad = jnp.zeros((96, 128), jnp.int32)
    turned = jnp.concatenate([slot_v[...], pad], axis=0).T
    lane16 = lax.broadcasted_iota(jnp.int32, (128, 128), 1).astype(I16)
    table = []
    for r in range(32):
        c = jnp.broadcast_to(turned[:, r : r + 1], (128, 128))
        colb[128 * r : 128 * r + 128, :] = c
        b1[128 * r : 128 * r + 128, :] = onehot((c % 128).astype(I16) == lane16)
        high = jnp.broadcast_to(slot_v[r : r + 1, :] // 128, (32, 128)).astype(I16)
        table.append(onehot(high == iota32.astype(I16)))
    counts = jnp.dot(jnp.concatenate(table, axis=1), b1[...], preferred_element_type=F32)
    in_targets.wait()
    targ = targ_v[...].astype(F32)
    lane = lax.broadcasted_iota(jnp.int32, (32, 128), 1)
    for m in range(4):
        t = pltpu.roll(targ, (128 - 32 * m) % 128, 1)
        c = pltpu.roll(counts, (128 + 32 - 32 * m) % 128, 1)
        v = jnp.where(lane < 32, t, jnp.where(lane < 64, c, 0.0))
        small[pl.ds(m, 32, stride=4), :] = v

    for n in range(4):
        in_raster[n].wait()
        for h in range(4):
            a = n * quarter + h * 256
            hi, lo = split(acc[a : a + 256, :])
            x2[a : a + 256, 0:128] = hi
            x2[a : a + 256, 128:256] = lo

    def sum_batch(b):
        g, bb = lax.div(b, 8), lax.rem(b, 8)
        places = [place(pick(CODES[k::8], bb), 1) + (g,) for k in range(BLK)]
        ids = jnp.concatenate([(iota32 + lin(*t) * CAP).astype(I16) for t in places], axis=0)
        table = [onehot(over_rows(slot_v[r : r + 1, :]) == ids) for r in range(32)]
        s = jnp.dot(jnp.concatenate(table, axis=1), x2[...], preferred_element_type=F32)
        s = s[:, :128] + s[:, 128:]
        for k in range(BLK):
            at = (b * 8 + k) * STEP
            send[pl.ds(pl.multiple_of(at, 8), CAP), :] = s[k * CAP : k * CAP + CAP, :]
            send[pl.ds(at + CAP, 1), :] = small[pl.ds(lin(*places[k]), 1), :]

    def send_batch(b):
        g, bb = lax.div(b, 8), lax.rem(b, 8)
        for k in range(BLK):
            i = bb * 8 + k
            t = place(pick(CODES[k::8], bb), 1) + (g,)
            src = send.at[pl.ds(pl.multiple_of((b * 8 + k) * STEP, 8), MSG)]
            dst = got.at[pl.ds(pl.multiple_of((core * 64 + i) * STEP, 8), MSG)]
            send_or_keep(src, dst, s_send.at[0], s_got.at[core * 8 + bb], t, k == 7)

    def first(b, carry):
        sum_batch(b)
        return carry

    def then_send(b, carry):
        send_batch(b)
        return carry

    lax.fori_loop(0, EARLY, first, 0)
    pl.semaphore_wait(barrier, DEVS - 1)
    lax.fori_loop(0, EARLY, then_send, 0)

    def batch(b, carry):
        sum_batch(b)
        send_batch(b)
        return carry

    lax.fori_loop(EARLY, BATCHES, batch, 0)

    for n in range(4):
        part = slice(n * 256, n * 256 + 256)
        tot[part, :] = jnp.zeros((256, 128), F32)
        num[part, :] = jnp.zeros((256, 128), F32)
    iota256 = lax.broadcasted_iota(jnp.int32, (256, 128), 0)
    sub8 = lax.broadcasted_iota(jnp.int32, (8, 128), 0)
    lane8 = lax.broadcasted_iota(jnp.int32, (8, 128), 1)

    def in_lanes(v, first):
        w = jnp.zeros((8, 128), F32)
        for m in range(4):
            here = (lane8 // 32 == m) & (sub8 % 4 == m)
            w = jnp.where(here, pltpu.roll(v, (128 + 32 * m - first) % 128, 1), w)
        return [jnp.sum(w[4 * h : 4 * h + 4, :], axis=0, keepdims=True) for h in range(2)]

    def gather_sums(n, carry):
        b = (n % 2) * 8 + n // 2
        at = b * BLK * STEP
        wait_bytes(got.at[pl.ds(pl.multiple_of(at, 8), BLK * MSG)], s_got.at[b])
        block = [got[pl.ds(pl.multiple_of(at + k * STEP, 8), CAP), :] for k in range(BLK)]
        r2 = jnp.concatenate(split(jnp.concatenate(block, axis=0)), axis=1)
        extra = [got[pl.ds(at + k * STEP + CAP, 1), :] for k in range(BLK)]
        extra = jnp.concatenate(extra, axis=0)
        wanted = [v.astype(jnp.int32) for v in in_lanes(extra, 0)]
        counts = in_lanes(extra, CAP)
        turned = jnp.concatenate(wanted + [jnp.zeros((6, 128), jnp.int32)], axis=0).T
        for h in range(2):
            column = jnp.broadcast_to(turned[:, h : h + 1], (128, 128))
            tcol[pl.ds(pl.multiple_of(b * ROWS + h * 128, 128), 128), :] = column
        rows = [over_rows(v) for v in wanted]
        for n in range(4):
            part = slice(n * 256, n * 256 + 256)
            ids = iota256 + n * 256
            c = num[part, :]
            for h in range(2):
                c = c + jnp.where(wanted[h] == ids, counts[h], 0.0)
            num[part, :] = c
            table = jnp.concatenate([onehot(v == ids.astype(I16)) for v in rows], axis=1)
            s = jnp.dot(table, r2, preferred_element_type=F32)
            tot[part, :] += s[:, :128] + s[:, 128:]
        return carry

    lax.fori_loop(0, BATCHES, gather_sums, 0)

    for n in range(4):
        part = slice(n * 256, n * 256 + 256)
        number = jnp.sum(num[part, :], axis=1, keepdims=True)
        mean = tot[part, :] * (1.0 / jnp.maximum(number, 1.0))
        tot[part, :] = mean
        hi, lo = split(mean)
        m2[part, 0:128] = hi
        m2[part, 128:256] = lo

    lane256 = lax.broadcasted_iota(jnp.int32, (256, 128), 1)

    def reply(n, carry):
        g, bb = (core + n // 8) % 2, n % 8
        b = g * 8 + bb
        here = pl.ds(pl.multiple_of(b * ROWS, ROWS), ROWS)
        wanted = tcol[here, :].astype(I16)
        table = jnp.concatenate(
            [onehot(wanted == (lane256 + 128 * n).astype(I16)) for n in range(8)], axis=1
        )
        s = jnp.dot(table, m2[...], preferred_element_type=F32)
        rep[here, :] = s[:, :128] + s[:, 128:]
        for k in range(BLK):
            i = bb * 8 + k
            t = place(pick(CODES[k::8], bb), -1) + (g,)
            src = rep.at[pl.ds(pl.multiple_of((b * 8 + k) * CAP, CAP), CAP)]
            dst = ret.at[pl.ds(pl.multiple_of((core * 64 + i) * CAP, CAP), CAP)]
            send_or_keep(src, dst, s_send.at[1], s_ret.at[core * 8 + bb], t, k == 7)
        return carry

    lax.fori_loop(0, BATCHES, reply, 0)

    lane1 = lax.broadcasted_iota(jnp.int32, (1, 128), 1)

    def subtract(n, r2, ids):
        part = pl.ds(pl.multiple_of(n * 256, 256), 256)
        px = colb[part, :].astype(I16)
        table = jnp.concatenate([onehot(px == v) for v in ids], axis=1)
        s = jnp.dot(table, r2, preferred_element_type=F32)
        acc[part, :] = acc[part, :] - s[:, :128] - s[:, 128:]

    def read_batch(b, carry):
        here = pl.ds(pl.multiple_of(b * ROWS, ROWS), ROWS)
        g, bb = lax.div(b, 8), lax.rem(b, 8)
        ids = []
        for h in range(2):
            v = lane1 % 32
            for m in range(4):
                base = lin(*place(pick(CODES[4 * h + m :: 8], bb), 1), g) * CAP
                v = v + jnp.where(lane1 // 32 == m, base, 0)
            ids.append(over_rows(v))
        wait_bytes(ret.at[here], s_ret.at[b])
        r2 = jnp.concatenate(split(ret[here, :]), axis=1)
        for n in range(16):
            subtract(n, r2, ids)
        return carry

    lax.fori_loop(0, BATCHES, read_batch, 0)

    wait_bytes(send.at[pl.ds(0, (DEVS - 1) * MSG)], s_send.at[0])
    wait_bytes(rep.at[pl.ds(0, (DEVS - 1) * CAP)], s_send.at[1])


def per_device(raster, slot_of, slot_target):
    operands = (raster.reshape(PIX, BANDS), slot_of, slot_target.reshape(32, 128))
    here = pl.BlockSpec(memory_space=pltpu.VMEM)
    outside = pl.BlockSpec(memory_space=pltpu.HBM)
    table = pltpu.VMEM((PIX, BANDS), F32)
    means, anomaly = pl.pallas_call(
        kernel,
        out_shape=(
            jax.ShapeDtypeStruct((PAR_DEV, BANDS), F32),
            jax.ShapeDtypeStruct((PIX, BANDS), F32),
        ),
        in_specs=[outside] * 3,
        out_specs=(here, here),
        scratch_shapes=[
            pltpu.VMEM((PIX, 2 * BANDS), BF),
            pltpu.VMEM((PIX, 128), BF),
            pltpu.VMEM((PIX, 128), jnp.int32),
            pltpu.VMEM((PIX, 128), jnp.int32),
            pltpu.VMEM((PAR_DEV, BANDS), F32),
            pltpu.VMEM((PAR_DEV, 2 * BANDS), BF),
            pltpu.VMEM((DEVS * STEP, BANDS), F32),
            pltpu.VMEM((DEVS * STEP, BANDS), F32),
            table,
            table,
            pltpu.VMEM((DEVS, 128), F32),
            pltpu.VMEM((32, 128), jnp.int32),
            pltpu.VMEM((32, 128), jnp.int32),
            pltpu.SemaphoreType.DMA((6,)),
            pltpu.SemaphoreType.DMA((2,)),
            pltpu.SemaphoreType.DMA((BATCHES,)),
            pltpu.SemaphoreType.DMA((BATCHES,)),
        ],
        compiler_params=pltpu.CompilerParams(
            collective_id=0, has_side_effects=True, vmem_limit_bytes=48 * 2**20
        ),
    )(*(pltpu.with_memory_space_constraint(v, pltpu.HBM) for v in operands))
    return means, anomaly.reshape(raster.shape)


def solution(mesh):
    placed = (P("row", "col", None), P("row", "col"), P("row", "col", None))
    return jax.shard_map(
        per_device,
        mesh=mesh,
        in_specs=placed,
        out_specs=(P(("row", "col"), None), P("row", "col", None)),
        check_vma=False,
    )
```

```python
import itertools
import random

import jax
import jax.numpy as jnp
from jax import lax
from jax.experimental import pallas as pl
from jax.experimental.pallas import tpu as pltpu
from jax.sharding import PartitionSpec as P

MESH = pl.DeviceIdType.MESH
PIX = 4096
BANDS = 128
PAR_DEV = 1024
CAP = 32
MSG = CAP + 1
STEP = 40
DEVS = 128
BLK = 8
ROWS = BLK * CAP
BATCHES = DEVS // BLK
EARLY = 2
BF = jnp.bfloat16
F32 = jnp.float32
I16 = jnp.int16


ORDER = [d for d in itertools.product(range(4), repeat=3) if any(d)]
random.Random(0).shuffle(ORDER)
ORDER.append((0, 0, 0))
CODES = [d[0] + 4 * d[1] + 16 * d[2] for d in ORDER]


def pick(values, index):
    got = jnp.int32(values[0])
    for n, v in enumerate(values[1:], 1):
        got = jnp.where(index == n, jnp.int32(v), got)
    return got


def split(v):
    hi = v.astype(BF)
    lo = (v - hi.astype(F32)).astype(BF)
    return hi, lo


def onehot(mask):
    return jnp.where(mask, jnp.ones((), BF), jnp.zeros((), BF))


def over_rows(v):
    v = jnp.broadcast_to(v, (16, 128)).astype(I16)
    return jnp.concatenate([v] * 16, axis=0)


def subtract(out, acc, colb, ids, block, done=lambda n: None):
    r2 = jnp.concatenate(split(block), axis=1)
    rows = [over_rows(v) for v in ids]
    for n in range(16):
        part = slice(n * 256, n * 256 + 256)
        px = colb[part, :].astype(I16)
        table = jnp.concatenate([onehot(px == v) for v in rows], axis=1)
        s = jnp.dot(table, r2, preferred_element_type=F32)
        out[part, :] = acc[part, :] - s[:, :128] - s[:, 128:]
        done(n)


def finish(tot, acc, colb, ids, last, means_out, anom_out, res, sems):
    means = pltpu.make_async_copy(tot, means_out, sems.at[4])
    means.start()
    copies = []

    def done(n):
        if n % 4 == 3:
            part = pl.ds((n // 4) * 1024, 1024)
            copy = pltpu.make_async_copy(res.at[part], anom_out.at[part], sems.at[n // 4])
            copy.start()
            copies.append(copy)

    subtract(res, acc, colb, [ids[h : h + 1, :] for h in range(2)], last[...], done)
    for copy in copies:
        copy.wait()
    means.wait()


def kernel(
    raster, slots, targets, tot, acc, colb, ids_out, last_out,
    x2, b1, tcol, num, m2,
    send, got, rep, ret, small, slot_v, targ_v,
    s_in, s_send, s_got, s_ret,
):
    row, col = lax.axis_index("row"), lax.axis_index("col")
    x, y, z, core = col % 4, row // 2, col // 4, row % 2
    me = row * 16 + col

    def place(code, sign):
        dx, dy, dz = lax.rem(code, 4), lax.rem(lax.div(code, 4), 4), lax.div(code, 16)
        return tuple(lax.rem(v + sign * d + 4, 4) for v, d in ((x, dx), (y, dy), (z, dz)))

    def lin(tx, ty, tz, tc):
        return (ty * 2 + tc) * 16 + tz * 4 + tx

    def remote(src, dst, send_sem, recv_sem, t):
        tx, ty, tz, tc = t
        pltpu.make_async_remote_copy(
            src_ref=src, dst_ref=dst, send_sem=send_sem, recv_sem=recv_sem,
            device_id=(ty * 2 + tc, tz * 4 + tx), device_id_type=MESH,
        ).start()

    def send_or_keep(src, dst, send_sem, recv_sem, t, may_be_self):
        if not may_be_self:
            remote(src, dst, send_sem, recv_sem, t)
            return
        mine = lin(*t) == me

        @pl.when(jnp.logical_not(mine))
        def _():
            remote(src, dst, send_sem, recv_sem, t)

        @pl.when(mine)
        def _():
            pltpu.make_async_copy(src, dst, recv_sem).start()

    def wait_bytes(ref, sem):
        pltpu.make_async_copy(ref, ref, sem).wait()

    in_slots = pltpu.make_async_copy(slots, slot_v, s_in.at[0])
    in_targets = pltpu.make_async_copy(targets, targ_v, s_in.at[1])
    in_slots.start()
    in_targets.start()
    quarter = PIX // 4
    in_raster = []
    for n in range(4):
        part = pl.ds(n * quarter, quarter)
        in_raster.append(pltpu.make_async_copy(raster.at[part], acc.at[part], s_in.at[2 + n]))
        in_raster[-1].start()
    barrier = pltpu.get_barrier_semaphore()

    around = [(k + 10) % 16 for k in range(16)]

    def greet(n, carry):
        far = lax.rem(row + n, 8)
        for k in around:
            there = (far, lax.rem(col + k, 16))
            pl.semaphore_signal(barrier, inc=1, device_id=there, device_id_type=MESH)
        return carry

    lax.fori_loop(4, 8, greet, 0)
    lax.fori_loop(1, 4, greet, 0)
    for k in around:
        if k:
            there = (row, lax.rem(col + k, 16))
            pl.semaphore_signal(barrier, inc=1, device_id=there, device_id_type=MESH)

    in_slots.wait()
    iota32 = lax.broadcasted_iota(jnp.int32, (32, 128), 0)

    pad = jnp.zeros((96, 128), jnp.int32)
    turned = jnp.concatenate([slot_v[...], pad], axis=0).T
    lane16 = lax.broadcasted_iota(jnp.int32, (128, 128), 1).astype(I16)
    table = []
    for r in range(32):
        c = jnp.broadcast_to(turned[:, r : r + 1], (128, 128))
        colb[128 * r : 128 * r + 128, :] = c
        b1[128 * r : 128 * r + 128, :] = onehot((c % 128).astype(I16) == lane16)
        high = jnp.broadcast_to(slot_v[r : r + 1, :] // 128, (32, 128)).astype(I16)
        table.append(onehot(high == iota32.astype(I16)))
    counts = jnp.dot(jnp.concatenate(table, axis=1), b1[...], preferred_element_type=F32)
    in_targets.wait()
    targ = targ_v[...].astype(F32)
    lane = lax.broadcasted_iota(jnp.int32, (32, 128), 1)
    for m in range(4):
        t = pltpu.roll(targ, (128 - 32 * m) % 128, 1)
        c = pltpu.roll(counts, (128 + 32 - 32 * m) % 128, 1)
        v = jnp.where(lane < 32, t, jnp.where(lane < 64, c, 0.0))
        small[pl.ds(m, 32, stride=4), :] = v

    for n in range(4):
        in_raster[n].wait()
        for h in range(4):
            a = n * quarter + h * 256
            hi, lo = split(acc[a : a + 256, :])
            x2[a : a + 256, 0:128] = hi
            x2[a : a + 256, 128:256] = lo

    def sum_batch(b):
        g, bb = lax.div(b, 8), lax.rem(b, 8)
        places = [place(pick(CODES[k::8], bb), 1) + (g,) for k in range(BLK)]
        ids = jnp.concatenate([(iota32 + lin(*t) * CAP).astype(I16) for t in places], axis=0)
        table = [onehot(over_rows(slot_v[r : r + 1, :]) == ids) for r in range(32)]
        s = jnp.dot(jnp.concatenate(table, axis=1), x2[...], preferred_element_type=F32)
        s = s[:, :128] + s[:, 128:]
        for k in range(BLK):
            at = (b * 8 + k) * STEP
            send[pl.ds(pl.multiple_of(at, 8), CAP), :] = s[k * CAP : k * CAP + CAP, :]
            send[pl.ds(at + CAP, 1), :] = small[pl.ds(lin(*places[k]), 1), :]

    def send_batch(b):
        g, bb = lax.div(b, 8), lax.rem(b, 8)
        for k in range(BLK):
            i = bb * 8 + k
            t = place(pick(CODES[k::8], bb), 1) + (g,)
            src = send.at[pl.ds(pl.multiple_of((b * 8 + k) * STEP, 8), MSG)]
            dst = got.at[pl.ds(pl.multiple_of((core * 64 + i) * STEP, 8), MSG)]
            send_or_keep(src, dst, s_send.at[0], s_got.at[core * 8 + bb], t, k == 7)

    def first(b, carry):
        sum_batch(b)
        return carry

    def then_send(b, carry):
        send_batch(b)
        return carry

    lax.fori_loop(0, EARLY, first, 0)
    pl.semaphore_wait(barrier, DEVS - 1)
    lax.fori_loop(0, EARLY, then_send, 0)

    def batch(b, carry):
        sum_batch(b)
        send_batch(b)
        return carry

    lax.fori_loop(EARLY, BATCHES, batch, 0)

    for n in range(4):
        part = slice(n * 256, n * 256 + 256)
        tot[part, :] = jnp.zeros((256, 128), F32)
        num[part, :] = jnp.zeros((256, 128), F32)
    iota256 = lax.broadcasted_iota(jnp.int32, (256, 128), 0)
    sub8 = lax.broadcasted_iota(jnp.int32, (8, 128), 0)
    lane8 = lax.broadcasted_iota(jnp.int32, (8, 128), 1)

    def in_lanes(v, first):
        w = jnp.zeros((8, 128), F32)
        for m in range(4):
            here = (lane8 // 32 == m) & (sub8 % 4 == m)
            w = jnp.where(here, pltpu.roll(v, (128 + 32 * m - first) % 128, 1), w)
        return [jnp.sum(w[4 * h : 4 * h + 4, :], axis=0, keepdims=True) for h in range(2)]

    def gather_sums(n, carry):
        b = (n % 2) * 8 + n // 2
        at = b * BLK * STEP
        wait_bytes(got.at[pl.ds(pl.multiple_of(at, 8), BLK * MSG)], s_got.at[b])
        block = [got[pl.ds(pl.multiple_of(at + k * STEP, 8), CAP), :] for k in range(BLK)]
        r2 = jnp.concatenate(split(jnp.concatenate(block, axis=0)), axis=1)
        extra = [got[pl.ds(at + k * STEP + CAP, 1), :] for k in range(BLK)]
        extra = jnp.concatenate(extra, axis=0)
        wanted = [v.astype(jnp.int32) for v in in_lanes(extra, 0)]
        counts = in_lanes(extra, CAP)
        turned = jnp.concatenate(wanted + [jnp.zeros((6, 128), jnp.int32)], axis=0).T
        for h in range(2):
            column = jnp.broadcast_to(turned[:, h : h + 1], (128, 128))
            tcol[pl.ds(pl.multiple_of(b * ROWS + h * 128, 128), 128), :] = column
        rows = [over_rows(v) for v in wanted]
        for n in range(4):
            part = slice(n * 256, n * 256 + 256)
            ids = iota256 + n * 256
            c = num[part, :]
            for h in range(2):
                c = c + jnp.where(wanted[h] == ids, counts[h], 0.0)
            num[part, :] = c
            table = jnp.concatenate([onehot(v == ids.astype(I16)) for v in rows], axis=1)
            s = jnp.dot(table, r2, preferred_element_type=F32)
            tot[part, :] += s[:, :128] + s[:, 128:]
        return carry

    lax.fori_loop(0, BATCHES, gather_sums, 0)

    for n in range(4):
        part = slice(n * 256, n * 256 + 256)
        number = jnp.sum(num[part, :], axis=1, keepdims=True)
        mean = tot[part, :] * (1.0 / jnp.maximum(number, 1.0))
        tot[part, :] = mean
        hi, lo = split(mean)
        m2[part, 0:128] = hi
        m2[part, 128:256] = lo

    lane256 = lax.broadcasted_iota(jnp.int32, (256, 128), 1)

    def reply(n, carry):
        g, bb = (core + n // 8) % 2, n % 8
        b = g * 8 + bb
        here = pl.ds(pl.multiple_of(b * ROWS, ROWS), ROWS)
        wanted = tcol[here, :].astype(I16)
        table = jnp.concatenate(
            [onehot(wanted == (lane256 + 128 * n).astype(I16)) for n in range(8)], axis=1
        )
        s = jnp.dot(table, m2[...], preferred_element_type=F32)
        rep[here, :] = s[:, :128] + s[:, 128:]
        for k in range(BLK):
            i = bb * 8 + k
            t = place(pick(CODES[k::8], bb), -1) + (g,)
            src = rep.at[pl.ds(pl.multiple_of((b * 8 + k) * CAP, CAP), CAP)]
            dst = ret.at[pl.ds(pl.multiple_of((core * 64 + i) * CAP, CAP), CAP)]
            send_or_keep(src, dst, s_send.at[1], s_ret.at[core * 8 + bb], t, k == 7)
        return carry

    lax.fori_loop(0, BATCHES, reply, 0)

    lane1 = lax.broadcasted_iota(jnp.int32, (1, 128), 1)

    def fetch(b):
        here = pl.ds(pl.multiple_of(b * ROWS, ROWS), ROWS)
        g, bb = lax.div(b, 8), lax.rem(b, 8)
        ids = []
        for h in range(2):
            v = lane1 % 32
            for m in range(4):
                base = lin(*place(pick(CODES[4 * h + m :: 8], bb), 1), g) * CAP
                v = v + jnp.where(lane1 // 32 == m, base, 0)
            ids.append(v)
        wait_bytes(ret.at[here], s_ret.at[b])
        return ids, ret[here, :]

    def read_batch(b, carry):
        ids, block = fetch(b)
        subtract(acc, acc, colb, ids, block)
        return carry

    lax.fori_loop(0, BATCHES - 1, read_batch, 0)
    ids, block = fetch(jnp.int32(BATCHES - 1))
    for h in range(2):
        ids_out[h : h + 1, :] = ids[h]
    last_out[...] = block

    wait_bytes(send.at[pl.ds(0, (DEVS - 1) * MSG)], s_send.at[0])
    wait_bytes(rep.at[pl.ds(0, (DEVS - 1) * CAP)], s_send.at[1])


def per_device(raster, slot_of, slot_target):
    operands = (raster.reshape(PIX, BANDS), slot_of, slot_target.reshape(32, 128))
    here = pl.BlockSpec(memory_space=pltpu.VMEM)
    outside = pl.BlockSpec(memory_space=pltpu.HBM)
    table = pltpu.VMEM((PIX, BANDS), F32)
    partial = pl.pallas_call(
        kernel,
        out_shape=(
            jax.ShapeDtypeStruct((PAR_DEV, BANDS), F32),
            jax.ShapeDtypeStruct((PIX, BANDS), F32),
            jax.ShapeDtypeStruct((PIX, 128), jnp.int32),
            jax.ShapeDtypeStruct((8, 128), jnp.int32),
            jax.ShapeDtypeStruct((ROWS, BANDS), F32),
        ),
        in_specs=[outside] * 3,
        out_specs=(here,) * 5,
        scratch_shapes=[
            pltpu.VMEM((PIX, 2 * BANDS), BF),
            pltpu.VMEM((PIX, 128), BF),
            pltpu.VMEM((PIX, 128), jnp.int32),
            pltpu.VMEM((PAR_DEV, BANDS), F32),
            pltpu.VMEM((PAR_DEV, 2 * BANDS), BF),
            pltpu.VMEM((DEVS * STEP, BANDS), F32),
            pltpu.VMEM((DEVS * STEP, BANDS), F32),
            table,
            table,
            pltpu.VMEM((DEVS, 128), F32),
            pltpu.VMEM((32, 128), jnp.int32),
            pltpu.VMEM((32, 128), jnp.int32),
            pltpu.SemaphoreType.DMA((6,)),
            pltpu.SemaphoreType.DMA((2,)),
            pltpu.SemaphoreType.DMA((BATCHES,)),
            pltpu.SemaphoreType.DMA((BATCHES,)),
        ],
        compiler_params=pltpu.CompilerParams(
            collective_id=0, has_side_effects=True, vmem_limit_bytes=48 * 2**20
        ),
    )(*(pltpu.with_memory_space_constraint(v, pltpu.HBM) for v in operands))
    means, anomaly = pl.pallas_call(
        finish,
        out_shape=(
            jax.ShapeDtypeStruct((PAR_DEV, BANDS), F32),
            jax.ShapeDtypeStruct((PIX, BANDS), F32),
        ),
        in_specs=[here] * 5,
        out_specs=(outside, outside),
        scratch_shapes=[table, pltpu.SemaphoreType.DMA((5,))],
        compiler_params=pltpu.CompilerParams(vmem_limit_bytes=16 * 2**20),
    )(*partial)
    return means, anomaly.reshape(raster.shape)


def solution(mesh):
    placed = (P("row", "col", None), P("row", "col"), P("row", "col", None))
    return jax.shard_map(
        per_device,
        mesh=mesh,
        in_specs=placed,
        out_specs=(P(("row", "col"), None), P("row", "col", None)),
        check_vma=False,
    )
```

```python
import itertools

import jax
import jax.numpy as jnp
from jax import lax
from jax.experimental import pallas as pl
from jax.experimental.pallas import tpu as pltpu
from jax.sharding import PartitionSpec as P

MESH = pl.DeviceIdType.MESH
PIX = 4096
BANDS = 128
PAR_DEV = 1024
CAP = 32
MSG = CAP + 1
STEP = 40
DEVS = 128
BLK = 8
ROWS = BLK * CAP
BATCHES = DEVS // BLK
EARLY = 2
BF = jnp.bfloat16
F32 = jnp.float32
I16 = jnp.int16


SHIFTS = list(itertools.product(range(4), repeat=2))
ORDER = [(t, (t + u) % 4, (t + v) % 4) for u, v in SHIFTS[1:] + SHIFTS[:1] for t in (2, 1, 3, 0)]
CODES = [d[0] + 4 * d[1] + 16 * d[2] for d in ORDER]


def pick(values, index):
    got = jnp.int32(values[0])
    for n, v in enumerate(values[1:], 1):
        got = jnp.where(index == n, jnp.int32(v), got)
    return got


def split(v):
    hi = v.astype(BF)
    lo = (v - hi.astype(F32)).astype(BF)
    return hi, lo


def onehot(mask):
    return jnp.where(mask, jnp.ones((), BF), jnp.zeros((), BF))


def over_rows(v):
    v = jnp.broadcast_to(v, (16, 128)).astype(I16)
    return jnp.concatenate([v] * 16, axis=0)


def subtract(out, acc, colb, ids, block, done=lambda n: None):
    r2 = jnp.concatenate(split(block), axis=1)
    rows = [over_rows(v) for v in ids]
    for n in range(16):
        part = slice(n * 256, n * 256 + 256)
        px = colb[part, :].astype(I16)
        table = jnp.concatenate([onehot(px == v) for v in rows], axis=1)
        s = jnp.dot(table, r2, preferred_element_type=F32)
        out[part, :] = acc[part, :] - s[:, :128] - s[:, 128:]
        done(n)


def finish(tot, acc, colb, ids, last, means_out, anom_out, res, sems):
    means = pltpu.make_async_copy(tot, means_out, sems.at[4])
    means.start()
    copies = []

    def done(n):
        if n % 4 == 3:
            part = pl.ds((n // 4) * 1024, 1024)
            copy = pltpu.make_async_copy(res.at[part], anom_out.at[part], sems.at[n // 4])
            copy.start()
            copies.append(copy)

    subtract(res, acc, colb, [ids[h : h + 1, :] for h in range(2)], last[...], done)
    for copy in copies:
        copy.wait()
    means.wait()


def kernel(
    raster, slots, targets, tot, acc, colb, ids_out, last_out,
    x2, b1, tcol, num, m2,
    send, got, rep, ret, small, slot_v, targ_v,
    s_in, s_send, s_got, s_ret,
):
    row, col = lax.axis_index("row"), lax.axis_index("col")
    x, y, z, core = col % 4, row // 2, col // 4, row % 2
    me = row * 16 + col

    def place(code, sign):
        dx, dy, dz = lax.rem(code, 4), lax.rem(lax.div(code, 4), 4), lax.div(code, 16)
        return tuple(lax.rem(v + sign * d + 4, 4) for v, d in ((x, dx), (y, dy), (z, dz)))

    def lin(tx, ty, tz, tc):
        return (ty * 2 + tc) * 16 + tz * 4 + tx

    def remote(src, dst, send_sem, recv_sem, t):
        tx, ty, tz, tc = t
        pltpu.make_async_remote_copy(
            src_ref=src, dst_ref=dst, send_sem=send_sem, recv_sem=recv_sem,
            device_id=(ty * 2 + tc, tz * 4 + tx), device_id_type=MESH,
        ).start()

    def send_or_keep(src, dst, send_sem, recv_sem, t, may_be_self):
        if not may_be_self:
            remote(src, dst, send_sem, recv_sem, t)
            return
        mine = lin(*t) == me

        @pl.when(jnp.logical_not(mine))
        def _():
            remote(src, dst, send_sem, recv_sem, t)

        @pl.when(mine)
        def _():
            pltpu.make_async_copy(src, dst, recv_sem).start()

    def wait_bytes(ref, sem):
        pltpu.make_async_copy(ref, ref, sem).wait()

    in_slots = pltpu.make_async_copy(slots, slot_v, s_in.at[0])
    in_targets = pltpu.make_async_copy(targets, targ_v, s_in.at[1])
    in_slots.start()
    in_targets.start()
    quarter = PIX // 4
    in_raster = []
    for n in range(4):
        part = pl.ds(n * quarter, quarter)
        in_raster.append(pltpu.make_async_copy(raster.at[part], acc.at[part], s_in.at[2 + n]))
        in_raster[-1].start()
    barrier = pltpu.get_barrier_semaphore()

    def greet(n, carry):
        far = (row + n) % 8
        for k in range(16):
            there = (far, (col + k) % 16)
            pl.semaphore_signal(barrier, inc=1, device_id=there, device_id_type=MESH)
        return carry

    for k in range(1, 16):
        there = (row, (col + k) % 16)
        pl.semaphore_signal(barrier, inc=1, device_id=there, device_id_type=MESH)
    lax.fori_loop(1, 8, greet, 0)

    in_slots.wait()
    iota32 = lax.broadcasted_iota(jnp.int32, (32, 128), 0)

    pad = jnp.zeros((96, 128), jnp.int32)
    turned = jnp.concatenate([slot_v[...], pad], axis=0).T
    lane16 = lax.broadcasted_iota(jnp.int32, (128, 128), 1).astype(I16)
    table = []
    for r in range(32):
        c = jnp.broadcast_to(turned[:, r : r + 1], (128, 128))
        colb[128 * r : 128 * r + 128, :] = c
        b1[128 * r : 128 * r + 128, :] = onehot((c % 128).astype(I16) == lane16)
        high = jnp.broadcast_to(slot_v[r : r + 1, :] // 128, (32, 128)).astype(I16)
        table.append(onehot(high == iota32.astype(I16)))
    counts = jnp.dot(jnp.concatenate(table, axis=1), b1[...], preferred_element_type=F32)
    in_targets.wait()
    targ = targ_v[...].astype(F32)
    lane = lax.broadcasted_iota(jnp.int32, (32, 128), 1)
    for m in range(4):
        t = pltpu.roll(targ, (128 - 32 * m) % 128, 1)
        c = pltpu.roll(counts, (128 + 32 - 32 * m) % 128, 1)
        v = jnp.where(lane < 32, t, jnp.where(lane < 64, c, 0.0))
        small[pl.ds(m, 32, stride=4), :] = v

    for n in range(4):
        in_raster[n].wait()
        for h in range(4):
            a = n * quarter + h * 256
            hi, lo = split(acc[a : a + 256, :])
            x2[a : a + 256, 0:128] = hi
            x2[a : a + 256, 128:256] = lo

    def sum_batch(b):
        g, bb = lax.div(b, 8), lax.rem(b, 8)
        places = [place(pick(CODES[k::8], bb), 1) + (g,) for k in range(BLK)]
        ids = jnp.concatenate([(iota32 + lin(*t) * CAP).astype(I16) for t in places], axis=0)
        table = [onehot(over_rows(slot_v[r : r + 1, :]) == ids) for r in range(32)]
        s = jnp.dot(jnp.concatenate(table, axis=1), x2[...], preferred_element_type=F32)
        s = s[:, :128] + s[:, 128:]
        for k in range(BLK):
            at = (b * 8 + k) * STEP
            send[pl.ds(pl.multiple_of(at, 8), CAP), :] = s[k * CAP : k * CAP + CAP, :]
            send[pl.ds(at + CAP, 1), :] = small[pl.ds(lin(*places[k]), 1), :]

    def send_batch(b):
        g, bb = lax.div(b, 8), lax.rem(b, 8)
        for k in range(BLK):
            i = bb * 8 + k
            t = place(pick(CODES[k::8], bb), 1) + (g,)
            src = send.at[pl.ds(pl.multiple_of((b * 8 + k) * STEP, 8), MSG)]
            dst = got.at[pl.ds(pl.multiple_of((core * 64 + i) * STEP, 8), MSG)]
            send_or_keep(src, dst, s_send.at[0], s_got.at[core * 8 + bb], t, k == 7)

    def first(b, carry):
        sum_batch(b)
        return carry

    def then_send(b, carry):
        send_batch(b)
        return carry

    lax.fori_loop(0, EARLY, first, 0)
    pl.semaphore_wait(barrier, DEVS - 1)
    lax.fori_loop(0, EARLY, then_send, 0)

    def batch(b, carry):
        sum_batch(b)
        send_batch(b)
        return carry

    lax.fori_loop(EARLY, BATCHES, batch, 0)

    for n in range(4):
        part = slice(n * 256, n * 256 + 256)
        tot[part, :] = jnp.zeros((256, 128), F32)
        num[part, :] = jnp.zeros((256, 128), F32)
    iota256 = lax.broadcasted_iota(jnp.int32, (256, 128), 0)
    sub8 = lax.broadcasted_iota(jnp.int32, (8, 128), 0)
    lane8 = lax.broadcasted_iota(jnp.int32, (8, 128), 1)

    def in_lanes(v, first):
        w = jnp.zeros((8, 128), F32)
        for m in range(4):
            here = (lane8 // 32 == m) & (sub8 % 4 == m)
            w = jnp.where(here, pltpu.roll(v, (128 + 32 * m - first) % 128, 1), w)
        return [jnp.sum(w[4 * h : 4 * h + 4, :], axis=0, keepdims=True) for h in range(2)]

    def gather_sums(n, carry):
        b = (n % 2) * 8 + n // 2
        at = b * BLK * STEP
        wait_bytes(got.at[pl.ds(pl.multiple_of(at, 8), BLK * MSG)], s_got.at[b])
        block = [got[pl.ds(pl.multiple_of(at + k * STEP, 8), CAP), :] for k in range(BLK)]
        r2 = jnp.concatenate(split(jnp.concatenate(block, axis=0)), axis=1)
        extra = [got[pl.ds(at + k * STEP + CAP, 1), :] for k in range(BLK)]
        extra = jnp.concatenate(extra, axis=0)
        wanted = [v.astype(jnp.int32) for v in in_lanes(extra, 0)]
        counts = in_lanes(extra, CAP)
        turned = jnp.concatenate(wanted + [jnp.zeros((6, 128), jnp.int32)], axis=0).T
        for h in range(2):
            column = jnp.broadcast_to(turned[:, h : h + 1], (128, 128))
            tcol[pl.ds(pl.multiple_of(b * ROWS + h * 128, 128), 128), :] = column
        rows = [over_rows(v) for v in wanted]
        for n in range(4):
            part = slice(n * 256, n * 256 + 256)
            ids = iota256 + n * 256
            c = num[part, :]
            for h in range(2):
                c = c + jnp.where(wanted[h] == ids, counts[h], 0.0)
            num[part, :] = c
            table = jnp.concatenate([onehot(v == ids.astype(I16)) for v in rows], axis=1)
            s = jnp.dot(table, r2, preferred_element_type=F32)
            tot[part, :] += s[:, :128] + s[:, 128:]
        return carry

    lax.fori_loop(0, BATCHES, gather_sums, 0)

    for n in range(4):
        part = slice(n * 256, n * 256 + 256)
        number = jnp.sum(num[part, :], axis=1, keepdims=True)
        mean = tot[part, :] * (1.0 / jnp.maximum(number, 1.0))
        tot[part, :] = mean
        hi, lo = split(mean)
        m2[part, 0:128] = hi
        m2[part, 128:256] = lo

    lane256 = lax.broadcasted_iota(jnp.int32, (256, 128), 1)

    def reply(n, carry):
        g, bb = (core + n // 8) % 2, n % 8
        b = g * 8 + bb
        here = pl.ds(pl.multiple_of(b * ROWS, ROWS), ROWS)
        wanted = tcol[here, :].astype(I16)
        table = jnp.concatenate(
            [onehot(wanted == (lane256 + 128 * n).astype(I16)) for n in range(8)], axis=1
        )
        s = jnp.dot(table, m2[...], preferred_element_type=F32)
        rep[here, :] = s[:, :128] + s[:, 128:]
        for k in range(BLK):
            i = bb * 8 + k
            t = place(pick(CODES[k::8], bb), -1) + (g,)
            src = rep.at[pl.ds(pl.multiple_of((b * 8 + k) * CAP, CAP), CAP)]
            dst = ret.at[pl.ds(pl.multiple_of((core * 64 + i) * CAP, CAP), CAP)]
            send_or_keep(src, dst, s_send.at[1], s_ret.at[core * 8 + bb], t, k == 7)
        return carry

    lax.fori_loop(0, BATCHES, reply, 0)

    lane1 = lax.broadcasted_iota(jnp.int32, (1, 128), 1)

    def fetch(b):
        here = pl.ds(pl.multiple_of(b * ROWS, ROWS), ROWS)
        g, bb = lax.div(b, 8), lax.rem(b, 8)
        ids = []
        for h in range(2):
            v = lane1 % 32
            for m in range(4):
                base = lin(*place(pick(CODES[4 * h + m :: 8], bb), 1), g) * CAP
                v = v + jnp.where(lane1 // 32 == m, base, 0)
            ids.append(v)
        wait_bytes(ret.at[here], s_ret.at[b])
        return ids, ret[here, :]

    def read_batch(b, carry):
        ids, block = fetch(b)
        subtract(acc, acc, colb, ids, block)
        return carry

    lax.fori_loop(0, BATCHES - 1, read_batch, 0)
    ids, block = fetch(jnp.int32(BATCHES - 1))
    for h in range(2):
        ids_out[h : h + 1, :] = ids[h]
    last_out[...] = block

    wait_bytes(send.at[pl.ds(0, (DEVS - 1) * MSG)], s_send.at[0])
    wait_bytes(rep.at[pl.ds(0, (DEVS - 1) * CAP)], s_send.at[1])


def per_device(raster, slot_of, slot_target):
    operands = (raster.reshape(PIX, BANDS), slot_of, slot_target.reshape(32, 128))
    here = pl.BlockSpec(memory_space=pltpu.VMEM)
    outside = pl.BlockSpec(memory_space=pltpu.HBM)
    table = pltpu.VMEM((PIX, BANDS), F32)
    partial = pl.pallas_call(
        kernel,
        out_shape=(
            jax.ShapeDtypeStruct((PAR_DEV, BANDS), F32),
            jax.ShapeDtypeStruct((PIX, BANDS), F32),
            jax.ShapeDtypeStruct((PIX, 128), jnp.int32),
            jax.ShapeDtypeStruct((8, 128), jnp.int32),
            jax.ShapeDtypeStruct((ROWS, BANDS), F32),
        ),
        in_specs=[outside] * 3,
        out_specs=(here,) * 5,
        scratch_shapes=[
            pltpu.VMEM((PIX, 2 * BANDS), BF),
            pltpu.VMEM((PIX, 128), BF),
            pltpu.VMEM((PIX, 128), jnp.int32),
            pltpu.VMEM((PAR_DEV, BANDS), F32),
            pltpu.VMEM((PAR_DEV, 2 * BANDS), BF),
            pltpu.VMEM((DEVS * STEP, BANDS), F32),
            pltpu.VMEM((DEVS * STEP, BANDS), F32),
            table,
            table,
            pltpu.VMEM((DEVS, 128), F32),
            pltpu.VMEM((32, 128), jnp.int32),
            pltpu.VMEM((32, 128), jnp.int32),
            pltpu.SemaphoreType.DMA((6,)),
            pltpu.SemaphoreType.DMA((2,)),
            pltpu.SemaphoreType.DMA((BATCHES,)),
            pltpu.SemaphoreType.DMA((BATCHES,)),
        ],
        compiler_params=pltpu.CompilerParams(
            collective_id=0, has_side_effects=True, vmem_limit_bytes=48 * 2**20
        ),
    )(*(pltpu.with_memory_space_constraint(v, pltpu.HBM) for v in operands))
    means, anomaly = pl.pallas_call(
        finish,
        out_shape=(
            jax.ShapeDtypeStruct((PAR_DEV, BANDS), F32),
            jax.ShapeDtypeStruct((PIX, BANDS), F32),
        ),
        in_specs=[here] * 5,
        out_specs=(outside, outside),
        scratch_shapes=[table, pltpu.SemaphoreType.DMA((5,))],
        compiler_params=pltpu.CompilerParams(vmem_limit_bytes=16 * 2**20),
    )(*partial)
    return means, anomaly.reshape(raster.shape)


def solution(mesh):
    placed = (P("row", "col", None), P("row", "col"), P("row", "col", None))
    return jax.shard_map(
        per_device,
        mesh=mesh,
        in_specs=placed,
        out_specs=(P(("row", "col"), None), P("row", "col", None)),
        check_vma=False,
    )
```

```python
import itertools
import random

import jax
import jax.numpy as jnp
from jax import lax
from jax.experimental import pallas as pl
from jax.experimental.pallas import tpu as pltpu
from jax.sharding import PartitionSpec as P

MESH = pl.DeviceIdType.MESH
PIX = 4096
BANDS = 128
PAR_DEV = 1024
CAP = 32
MSG = CAP + 1
STEP = 40
DEVS = 128
BLK = 8
ROWS = BLK * CAP
BATCHES = DEVS // BLK
EARLY = 1
BF = jnp.bfloat16
F32 = jnp.float32
I16 = jnp.int16


ORDER = [d for d in itertools.product(range(4), repeat=3) if any(d)]
random.Random(0).shuffle(ORDER)
ORDER.append((0, 0, 0))
CODES = [d[0] + 4 * d[1] + 16 * d[2] for d in ORDER]


def pick(values, index):
    got = jnp.int32(values[0])
    for n, v in enumerate(values[1:], 1):
        got = jnp.where(index == n, jnp.int32(v), got)
    return got


def split(v):
    hi = v.astype(BF)
    lo = (v - hi.astype(F32)).astype(BF)
    return hi, lo


def onehot(mask):
    return jnp.where(mask, jnp.ones((), BF), jnp.zeros((), BF))


def over_rows(v):
    v = jnp.broadcast_to(v, (16, 128)).astype(I16)
    return jnp.concatenate([v] * 16, axis=0)


def kernel(
    raster, slots, targets, tot, acc,
    x2, b1, colb, tcol, num, m2,
    send, got, rep, ret, small, slot_v, targ_v,
    s_in, s_send, s_got, s_ret,
):
    row, col = lax.axis_index("row"), lax.axis_index("col")
    x, y, z, core = col % 4, row // 2, col // 4, row % 2
    me = row * 16 + col

    def place(code, sign):
        dx, dy, dz = lax.rem(code, 4), lax.rem(lax.div(code, 4), 4), lax.div(code, 16)
        return tuple(lax.rem(v + sign * d + 4, 4) for v, d in ((x, dx), (y, dy), (z, dz)))

    def lin(tx, ty, tz, tc):
        return (ty * 2 + tc) * 16 + tz * 4 + tx

    def remote(src, dst, send_sem, recv_sem, t):
        tx, ty, tz, tc = t
        pltpu.make_async_remote_copy(
            src_ref=src, dst_ref=dst, send_sem=send_sem, recv_sem=recv_sem,
            device_id=(ty * 2 + tc, tz * 4 + tx), device_id_type=MESH,
        ).start()

    def send_or_keep(src, dst, send_sem, recv_sem, t, may_be_self):
        if not may_be_self:
            remote(src, dst, send_sem, recv_sem, t)
            return
        mine = lin(*t) == me

        @pl.when(jnp.logical_not(mine))
        def _():
            remote(src, dst, send_sem, recv_sem, t)

        @pl.when(mine)
        def _():
            pltpu.make_async_copy(src, dst, recv_sem).start()

    def wait_bytes(ref, sem):
        pltpu.make_async_copy(ref, ref, sem).wait()

    in_slots = pltpu.make_async_copy(slots, slot_v, s_in.at[0])
    in_targets = pltpu.make_async_copy(targets, targ_v, s_in.at[1])
    in_slots.start()
    in_targets.start()
    quarter = PIX // 4
    in_raster = []
    for n in range(4):
        part = pl.ds(n * quarter, quarter)
        in_raster.append(pltpu.make_async_copy(raster.at[part], acc.at[part], s_in.at[2 + n]))
        in_raster[-1].start()
    barrier = pltpu.get_barrier_semaphore()

    def greet(n, carry):
        far = (row + n) % 8
        for k in range(16):
            there = (far, (col + k) % 16)
            pl.semaphore_signal(barrier, inc=1, device_id=there, device_id_type=MESH)
        return carry

    for k in range(1, 16):
        there = (row, (col + k) % 16)
        pl.semaphore_signal(barrier, inc=1, device_id=there, device_id_type=MESH)
    lax.fori_loop(1, 8, greet, 0)

    in_slots.wait()
    iota32 = lax.broadcasted_iota(jnp.int32, (32, 128), 0)

    pad = jnp.zeros((96, 128), jnp.int32)
    turned = jnp.concatenate([slot_v[...], pad], axis=0).T
    lane16 = lax.broadcasted_iota(jnp.int32, (128, 128), 1).astype(I16)
    table = []
    for r in range(32):
        c = jnp.broadcast_to(turned[:, r : r + 1], (128, 128))
        colb[128 * r : 128 * r + 128, :] = c
        b1[128 * r : 128 * r + 128, :] = onehot((c % 128).astype(I16) == lane16)
        high = jnp.broadcast_to(slot_v[r : r + 1, :] // 128, (32, 128)).astype(I16)
        table.append(onehot(high == iota32.astype(I16)))
    counts = jnp.dot(jnp.concatenate(table, axis=1), b1[...], preferred_element_type=F32)
    in_targets.wait()
    targ = targ_v[...].astype(F32)
    lane = lax.broadcasted_iota(jnp.int32, (32, 128), 1)
    for m in range(4):
        t = pltpu.roll(targ, (128 - 32 * m) % 128, 1)
        c = pltpu.roll(counts, (128 + 32 - 32 * m) % 128, 1)
        v = jnp.where(lane < 32, t, jnp.where(lane < 64, c, 0.0))
        small[pl.ds(m, 32, stride=4), :] = v

    for n in range(4):
        in_raster[n].wait()
        for h in range(4):
            a = n * quarter + h * 256
            hi, lo = split(acc[a : a + 256, :])
            x2[a : a + 256, 0:128] = hi
            x2[a : a + 256, 128:256] = lo

    def sum_batch(b):
        g, bb = lax.div(b, 8), lax.rem(b, 8)
        places = [place(pick(CODES[k::8], bb), 1) + (g,) for k in range(BLK)]
        ids = jnp.concatenate([(iota32 + lin(*t) * CAP).astype(I16) for t in places], axis=0)
        table = [onehot(over_rows(slot_v[r : r + 1, :]) == ids) for r in range(32)]
        s = jnp.dot(jnp.concatenate(table, axis=1), x2[...], preferred_element_type=F32)
        s = s[:, :128] + s[:, 128:]
        for k in range(BLK):
            at = (b * 8 + k) * STEP
            send[pl.ds(pl.multiple_of(at, 8), CAP), :] = s[k * CAP : k * CAP + CAP, :]
            send[pl.ds(at + CAP, 1), :] = small[pl.ds(lin(*places[k]), 1), :]

    def send_batch(b):
        g, bb = lax.div(b, 8), lax.rem(b, 8)
        for k in range(BLK):
            i = bb * 8 + k
            t = place(pick(CODES[k::8], bb), 1) + (g,)
            src = send.at[pl.ds(pl.multiple_of((b * 8 + k) * STEP, 8), MSG)]
            dst = got.at[pl.ds(pl.multiple_of((core * 64 + i) * STEP, 8), MSG)]
            send_or_keep(src, dst, s_send.at[0], s_got.at[core * 8 + bb], t, k == 7)

    def first(b, carry):
        sum_batch(b)
        return carry

    def then_send(b, carry):
        send_batch(b)
        return carry

    lax.fori_loop(0, EARLY, first, 0)
    pl.semaphore_wait(barrier, DEVS - 1)
    lax.fori_loop(0, EARLY, then_send, 0)

    def batch(b, carry):
        sum_batch(b)
        send_batch(b)
        return carry

    lax.fori_loop(EARLY, BATCHES, batch, 0)

    for n in range(4):
        part = slice(n * 256, n * 256 + 256)
        tot[part, :] = jnp.zeros((256, 128), F32)
        num[part, :] = jnp.zeros((256, 128), F32)
    iota256 = lax.broadcasted_iota(jnp.int32, (256, 128), 0)
    sub8 = lax.broadcasted_iota(jnp.int32, (8, 128), 0)
    lane8 = lax.broadcasted_iota(jnp.int32, (8, 128), 1)

    def in_lanes(v, first):
        w = jnp.zeros((8, 128), F32)
        for m in range(4):
            here = (lane8 // 32 == m) & (sub8 % 4 == m)
            w = jnp.where(here, pltpu.roll(v, (128 + 32 * m - first) % 128, 1), w)
        return [jnp.sum(w[4 * h : 4 * h + 4, :], axis=0, keepdims=True) for h in range(2)]

    def gather_sums(n, carry):
        b = (n % 2) * 8 + n // 2
        at = b * BLK * STEP
        wait_bytes(got.at[pl.ds(pl.multiple_of(at, 8), BLK * MSG)], s_got.at[b])
        block = [got[pl.ds(pl.multiple_of(at + k * STEP, 8), CAP), :] for k in range(BLK)]
        r2 = jnp.concatenate(split(jnp.concatenate(block, axis=0)), axis=1)
        extra = [got[pl.ds(at + k * STEP + CAP, 1), :] for k in range(BLK)]
        extra = jnp.concatenate(extra, axis=0)
        wanted = [v.astype(jnp.int32) for v in in_lanes(extra, 0)]
        counts = in_lanes(extra, CAP)
        turned = jnp.concatenate(wanted + [jnp.zeros((6, 128), jnp.int32)], axis=0).T
        for h in range(2):
            column = jnp.broadcast_to(turned[:, h : h + 1], (128, 128))
            tcol[pl.ds(pl.multiple_of(b * ROWS + h * 128, 128), 128), :] = column
        rows = [over_rows(v) for v in wanted]
        for n in range(4):
            part = slice(n * 256, n * 256 + 256)
            ids = iota256 + n * 256
            c = num[part, :]
            for h in range(2):
                c = c + jnp.where(wanted[h] == ids, counts[h], 0.0)
            num[part, :] = c
            table = jnp.concatenate([onehot(v == ids.astype(I16)) for v in rows], axis=1)
            s = jnp.dot(table, r2, preferred_element_type=F32)
            tot[part, :] += s[:, :128] + s[:, 128:]
        return carry

    lax.fori_loop(0, BATCHES, gather_sums, 0)

    for n in range(4):
        part = slice(n * 256, n * 256 + 256)
        number = jnp.sum(num[part, :], axis=1, keepdims=True)
        mean = tot[part, :] * (1.0 / jnp.maximum(number, 1.0))
        tot[part, :] = mean
        hi, lo = split(mean)
        m2[part, 0:128] = hi
        m2[part, 128:256] = lo

    lane256 = lax.broadcasted_iota(jnp.int32, (256, 128), 1)

    def reply(n, carry):
        g, bb = (core + n // 8) % 2, n % 8
        b = g * 8 + bb
        here = pl.ds(pl.multiple_of(b * ROWS, ROWS), ROWS)
        wanted = tcol[here, :].astype(I16)
        table = jnp.concatenate(
            [onehot(wanted == (lane256 + 128 * n).astype(I16)) for n in range(8)], axis=1
        )
        s = jnp.dot(table, m2[...], preferred_element_type=F32)
        rep[here, :] = s[:, :128] + s[:, 128:]
        for k in range(BLK):
            i = bb * 8 + k
            t = place(pick(CODES[k::8], bb), -1) + (g,)
            src = rep.at[pl.ds(pl.multiple_of((b * 8 + k) * CAP, CAP), CAP)]
            dst = ret.at[pl.ds(pl.multiple_of((core * 64 + i) * CAP, CAP), CAP)]
            send_or_keep(src, dst, s_send.at[1], s_ret.at[core * 8 + bb], t, k == 7)
        return carry

    lax.fori_loop(0, BATCHES, reply, 0)

    lane1 = lax.broadcasted_iota(jnp.int32, (1, 128), 1)

    def subtract(n, r2, ids):
        part = pl.ds(pl.multiple_of(n * 256, 256), 256)
        px = colb[part, :].astype(I16)
        table = jnp.concatenate([onehot(px == v) for v in ids], axis=1)
        s = jnp.dot(table, r2, preferred_element_type=F32)
        acc[part, :] = acc[part, :] - s[:, :128] - s[:, 128:]

    def read_batch(b, carry):
        here = pl.ds(pl.multiple_of(b * ROWS, ROWS), ROWS)
        g, bb = lax.div(b, 8), lax.rem(b, 8)
        ids = []
        for h in range(2):
            v = lane1 % 32
            for m in range(4):
                base = lin(*place(pick(CODES[4 * h + m :: 8], bb), 1), g) * CAP
                v = v + jnp.where(lane1 // 32 == m, base, 0)
            ids.append(over_rows(v))
        wait_bytes(ret.at[here], s_ret.at[b])
        r2 = jnp.concatenate(split(ret[here, :]), axis=1)
        for n in range(16):
            subtract(n, r2, ids)
        return carry

    lax.fori_loop(0, BATCHES, read_batch, 0)

    wait_bytes(send.at[pl.ds(0, (DEVS - 1) * MSG)], s_send.at[0])
    wait_bytes(rep.at[pl.ds(0, (DEVS - 1) * CAP)], s_send.at[1])


def per_device(raster, slot_of, slot_target):
    operands = (raster.reshape(PIX, BANDS), slot_of, slot_target.reshape(32, 128))
    here = pl.BlockSpec(memory_space=pltpu.VMEM)
    outside = pl.BlockSpec(memory_space=pltpu.HBM)
    table = pltpu.VMEM((PIX, BANDS), F32)
    means, anomaly = pl.pallas_call(
        kernel,
        out_shape=(
            jax.ShapeDtypeStruct((PAR_DEV, BANDS), F32),
            jax.ShapeDtypeStruct((PIX, BANDS), F32),
        ),
        in_specs=[outside] * 3,
        out_specs=(here, here),
        scratch_shapes=[
            pltpu.VMEM((PIX, 2 * BANDS), BF),
            pltpu.VMEM((PIX, 128), BF),
            pltpu.VMEM((PIX, 128), jnp.int32),
            pltpu.VMEM((PIX, 128), jnp.int32),
            pltpu.VMEM((PAR_DEV, BANDS), F32),
            pltpu.VMEM((PAR_DEV, 2 * BANDS), BF),
            pltpu.VMEM((DEVS * STEP, BANDS), F32),
            pltpu.VMEM((DEVS * STEP, BANDS), F32),
            table,
            table,
            pltpu.VMEM((DEVS, 128), F32),
            pltpu.VMEM((32, 128), jnp.int32),
            pltpu.VMEM((32, 128), jnp.int32),
            pltpu.SemaphoreType.DMA((6,)),
            pltpu.SemaphoreType.DMA((2,)),
            pltpu.SemaphoreType.DMA((BATCHES,)),
            pltpu.SemaphoreType.DMA((BATCHES,)),
        ],
        compiler_params=pltpu.CompilerParams(
            collective_id=0, has_side_effects=True, vmem_limit_bytes=48 * 2**20
        ),
    )(*(pltpu.with_memory_space_constraint(v, pltpu.HBM) for v in operands))
    return means, anomaly.reshape(raster.shape)


def solution(mesh):
    placed = (P("row", "col", None), P("row", "col"), P("row", "col", None))
    return jax.shard_map(
        per_device,
        mesh=mesh,
        in_specs=placed,
        out_specs=(P(("row", "col"), None), P("row", "col", None)),
        check_vma=False,
    )
```
